32 devices in a mesh: expert: 4 (over y, x), shard: 8 (over z, core).
Axes of the slice: x: 2, y: 2, z: 4, core: 2. Of those that a mesh axis runs over, the one named last changes fastest.
Arguments:
- master_gate: float32 [128, 2048, 768], P('expert', 'shard'), may hold values from -0.1875 to 0.1875
- second_gate: bfloat16 [128, 2048, 768], P('expert', 'shard'), may hold values from -0.0625 to 0.0625
- master_up: float32 [128, 2048, 768], P('expert', 'shard'), may hold values from -0.1875 to 0.1875
- second_up: bfloat16 [128, 2048, 768], P('expert', 'shard'), may hold values from -0.0625 to 0.0625
- router_weight: float32 [2048, 128], P('shard', 'expert'), may hold values from -0.125 to 0.125
- router_gain: float32 [2048], P('shard'), may hold values from 0.25 to 1.75
Outputs:
- final_gate: bfloat16 [128, 2048, 768], P(('expert', 'shard'))
- final_up: bfloat16 [128, 2048, 768], P(('expert', 'shard'))
- scale_gate: float32 [128, 768], P(('expert', 'shard'))
- scale_up: float32 [128, 768], P(('expert', 'shard'))
- serve_router: bfloat16 [2048, 128], replicated
The draws below stay inside these ranges and needn't reach their ends.
All inputs are finite; a program needn't handle non-finite values. Where the reference program divides by a largest or mean magnitude, that divisor is 1e-20 or more.
Results may differ from the reference program's by a relative error of at most 0.0085.
Values may be sent and summed in bfloat16 or wider, within the bound.
A program may use at most 192 MiB of HBM per device.

```python
import jax
import jax.numpy as jnp

EXPERTS = 128
D_MODEL = 2048
D_EXPERT = 768


def raised(entries, rng, source, target, shards_of, factor):
    def block_of(position):
        return (jnp.arange(entries.shape[position]) // (entries.shape[position] // shards_of)).reshape((-1,) + (1,) * (entries.ndim - 1 - position))

    first = jax.random.permutation(rng, shards_of)[block_of(target)]
    other_side = (block_of(target) + shards_of // 2) % shards_of
    return jnp.where((block_of(source) == first) | (block_of(source) == other_side), factor * entries, entries)


def block_levels(stream_key, extent, split, low, top_value):
    factor_of, own = 1.0, jax.random.fold_in(stream_key, 6)
    for dim, blocks in split:
        steps = jnp.exp(jax.random.uniform(jax.random.fold_in(own, dim), (blocks,), jnp.float32, low / len(split), top_value / len(split)))
        factor_of = factor_of * jnp.repeat(steps, extent[dim] // blocks).reshape([-1 if axis == dim else 1 for axis in range(len(extent))])
    return factor_of


def normal_values(own_key, dims, scale, bound, cuts=(), held_as=jnp.bfloat16):
    loudness = block_levels(own_key, dims, cuts, -0.22, 0.18) if cuts else 1.0
    result = jax.random.normal(own_key, dims, jnp.float32) * scale * loudness
    return jnp.minimum(jnp.maximum(result, -bound), bound).astype(held_as)


def noise_with(key, shape, width, most, split, heavy, dtype=jnp.bfloat16):
    entries = width * jax.random.normal(key, shape, jnp.float32)
    if split:
        entries = entries * block_levels(key, shape, split, -0.22, 0.18)
    return jnp.clip(raised(entries, jax.random.fold_in(key, 3), *heavy), -most, most).astype(dtype)


def setup_inputs(seed: int = 0) -> dict:
    key_of = jax.random.split(jax.random.key(seed), 7)
    master_gate = noise_with(key_of[0], (EXPERTS, D_MODEL, D_EXPERT), D_MODEL ** -0.5, 0.1875, ((0, 4), (1, 8)), (1, 2, 8, 2.0), jnp.float32)
    second_gate = normal_values(key_of[1], (EXPERTS, D_MODEL, D_EXPERT), (D_MODEL * 4) ** -0.5, 0.0625, ((0, 4), (1, 8)))
    master_up = noise_with(key_of[2], (EXPERTS, D_MODEL, D_EXPERT), D_MODEL ** -0.5, 0.1875, ((0, 4), (1, 8)), (1, 2, 8, 2.0), jnp.float32)
    second_up = normal_values(key_of[3], (EXPERTS, D_MODEL, D_EXPERT), (D_MODEL * 4) ** -0.5, 0.0625, ((0, 4), (1, 8)))
    router_weight = normal_values(key_of[4], (D_MODEL, EXPERTS), D_MODEL ** -0.5, 0.125, ((0, 8), (1, 4)), jnp.float32)
    router_gain = jnp.clip(1.0 + 0.15 * jax.random.normal(key_of[5], (D_MODEL,), jnp.float32), 0.25, 1.75)
    return {"master_gate": master_gate, "second_gate": second_gate, "master_up": master_up, "second_up": second_up, "router_weight": router_weight, "router_gain": router_gain}


def reference(master_gate, second_gate, master_up, second_up, router_weight, router_gain):
    merged_gate = master_gate + second_gate.astype(jnp.float32)
    merged_up = master_up + second_up.astype(jnp.float32)
    scale_gate = jnp.sum(jnp.abs(merged_gate), axis=1) / D_MODEL
    final_gate = (merged_gate / jnp.expand_dims(scale_gate, 1)).astype(jnp.bfloat16)
    scale_up = jnp.sum(jnp.abs(merged_up), axis=1) / D_MODEL
    final_up = (merged_up / jnp.expand_dims(scale_up, 1)).astype(jnp.bfloat16)
    serve_router = (router_weight * router_gain[:, None]).astype(jnp.bfloat16)
    return final_gate, final_up, scale_gate, scale_up, serve_router
```

```python
import functools

import jax
import jax.numpy as jnp
from jax import lax
from jax.experimental import pallas as pl
from jax.experimental.pallas import tpu as pltpu
from jax.sharding import PartitionSpec as P

MESH = pl.DeviceIdType.MESH
SLOTS = 3
STRIP = 64


def exchange(
    groups, n, each, rows, width,
    master_gate, second_gate, master_up, second_up, router,
    final_gate, final_up, scale_gate, scale_up, routed,
    land_gate, land_up, out_sem, sent, wide, narrow, in_sem, send_sem, recv_sem, row_send, row_recv, col_send, col_recv,
):
    group, me = lax.axis_index("expert"), lax.axis_index("shard")
    half = n // 2
    near = half - 2
    n_remote = each * (n - 1)
    n_items = each * n
    base = (me // half) * half
    chip = me // 2
    outer = ((chip == 0) | (chip == half - 1)).astype(jnp.int32)

    def item(i):
        cross_start = outer * (each * near)
        near_start = (1 - outer) * (each * half)
        is_cross = (i >= cross_start) & (i < cross_start + each * half)
        is_near = (i >= near_start) & (i < near_start + each * near)
        is_pair = (i >= each * (n - 2)) & (i < n_remote)
        q = i - cross_start
        cross_to = lax.rem(base + half + lax.rem(q + me + n_items, half), n)
        cross_j = q // half
        p = i - near_start
        near_to = base + lax.rem((me - base) // 2 * 2 + 2 + lax.rem(p + n_items * near, near), half)
        near_j = p // near
        pair_to = me + 1 - 2 * lax.rem(me, 2)
        pair_j = i - each * (n - 2)
        own_j = i - n_remote
        target = jnp.where(is_cross, cross_to, jnp.where(is_near, near_to, jnp.where(is_pair, pair_to, me)))
        j = jnp.where(is_cross, cross_j, jnp.where(is_near, near_j, jnp.where(is_pair, pair_j, own_j)))
        return target, j

    sources = ((master_gate, second_gate), (master_up, second_up))
    lands = (land_gate, land_up)

    def reads(i):
        target, j = item(i)
        slot = lax.rem(i, SLOTS)
        e = target * each + j
        return [
            pltpu.make_async_copy(ref.at[e], held.at[slot, t], in_sem.at[slot, t, k])
            for t in range(2)
            for k, (ref, held) in enumerate(zip(sources[t], (wide, narrow)))
        ]

    def my_rows():
        return pl.ds(pl.multiple_of(me * rows, rows), rows)

    def sends(i):
        target, j = item(i)
        return [
            pltpu.make_async_remote_copy(
                src_ref=sent.at[i, t],
                dst_ref=lands[t].at[j, my_rows()],
                send_sem=send_sem.at[i, t],
                recv_sem=recv_sem.at[j, t, me],
                device_id=(group, target),
                device_id_type=MESH,
            )
            for t in range(2)
        ]

    for i in range(SLOTS):
        for copy in reads(jnp.int32(i)):
            copy.start()

    barrier = pltpu.get_barrier_semaphore()
    for k in range(1, n):
        pl.semaphore_signal(barrier, inc=1, device_id=(group, lax.rem(me + k, n)), device_id_type=MESH)
    for k in range(1, groups):
        pl.semaphore_signal(barrier, inc=1, device_id=(lax.rem(group + k, groups), me), device_id_type=MESH)
    pl.semaphore_wait(barrier, n + groups - 2)

    def row_copy(k):
        return pltpu.make_async_remote_copy(
            src_ref=router,
            dst_ref=routed.at[group, :, my_rows()],
            send_sem=row_send.at[k],
            recv_sem=row_recv.at[k],
            device_id=(group, lax.rem(me + k + 1, n)),
            device_id_type=MESH,
        )

    def col_copy(k):
        return pltpu.make_async_remote_copy(
            src_ref=routed.at[group],
            dst_ref=routed.at[group],
            send_sem=col_send.at[k],
            recv_sem=col_recv.at[k],
            device_id=(lax.rem(group + k + 1, groups), me),
            device_id_type=MESH,
        )

    def merge(i, put):
        slot = lax.rem(i, SLOTS)
        for t in range(2):
            def strip(s, carry, t=t):
                at = pl.ds(pl.multiple_of(s * STRIP, STRIP), STRIP)
                total = wide[slot, t, at, :] + narrow[slot, t, at, :].astype(jnp.float32)
                put(t, s, total.astype(jnp.bfloat16))
                return carry
            lax.fori_loop(0, rows // STRIP, strip, 0)

    def produce(i, carry):
        for copy in reads(i):
            copy.wait()

        @pl.when(i < n_remote)
        def _():
            def put(t, s, value):
                sent[i, t, pl.ds(pl.multiple_of(s * STRIP, STRIP), STRIP), :] = value
            merge(i, put)

        @pl.when(i >= n_remote)
        def _():
            def put(t, s, value):
                lands[t][i - n_remote, pl.ds(pl.multiple_of(me * rows + s * STRIP, STRIP), STRIP), :] = value
            merge(i, put)

        @pl.when(i + SLOTS < n_items)
        def _():
            for copy in reads(i + SLOTS):
                copy.start()

        @pl.when((i >= 1) & (i <= n_remote))
        def _():
            for copy in sends(i - 1):
                copy.start()
        return carry

    lax.fori_loop(0, n_items, produce, 0)

    for k in range(n - 1):
        row_copy(k).start()
    routed[group, :, my_rows()] = router[...]
    for k in range(n - 1):
        row_copy(k).wait()
    for k in range(groups - 1):
        col_copy(k).start()

    scales = (scale_gate, scale_up)
    d_model = n * rows

    def put_out(j, t):
        return pltpu.make_async_copy(lands[t].at[j], (final_gate, final_up)[t].at[j], out_sem.at[j, t])

    def finish(j, carry):
        for t in range(2):
            land = lands[t]

            def arrive(k, c, t=t):
                source = lax.rem(me + 1 + k, n)
                pltpu.make_async_remote_copy(
                    src_ref=sent.at[0, t],
                    dst_ref=lands[t].at[j, pl.ds(pl.multiple_of(source * rows, rows), rows)],
                    send_sem=send_sem.at[0, t],
                    recv_sem=recv_sem.at[j, t, source],
                    device_id=(group, source),
                    device_id_type=MESH,
                ).wait_recv()
                return c

            lax.fori_loop(0, n - 1, arrive, 0)

            def add(s, total, land=land):
                at = pl.ds(pl.multiple_of(s * STRIP, STRIP), STRIP)
                block = jnp.abs(land[j, at, :].astype(jnp.float32))
                return total + jnp.sum(block.reshape(STRIP // 8, 8, width), axis=0)

            total = lax.fori_loop(0, d_model // STRIP, add, jnp.zeros((8, width), jnp.float32))
            scale = jnp.sum(total, axis=0, keepdims=True) / d_model
            scales[t][j] = scale
            factor = jnp.broadcast_to(1.0 / scale, (STRIP, width))

            def divide(s, c, land=land, factor=factor):
                at = pl.ds(pl.multiple_of(s * STRIP, STRIP), STRIP)
                land[j, at, :] = (land[j, at, :].astype(jnp.float32) * factor).astype(jnp.bfloat16)
                return c

            lax.fori_loop(0, d_model // STRIP, divide, 0)
            put_out(j, t).start()
        return carry

    lax.fori_loop(0, each, finish, 0)

    for k in range(groups - 1):
        col_copy(k).wait()

    def drain(i, carry):
        for copy in sends(i):
            copy.wait_send()
        return carry

    lax.fori_loop(0, n_remote, drain, 0)
    for j in range(each):
        for t in range(2):
            put_out(j, t).wait()


def shards(groups, n, master_gate, second_gate, master_up, second_up, router_weight, router_gain):
    experts, rows, width = master_gate.shape
    each = experts // n
    columns = router_weight.shape[1]
    router = (router_weight * router_gain[:, None]).astype(jnp.bfloat16).T
    land = pltpu.VMEM((each, n * rows, width), jnp.bfloat16)
    final = jax.ShapeDtypeStruct((each, n * rows, width), jnp.bfloat16)
    scale = jax.ShapeDtypeStruct((each, 1, width), jnp.float32)
    vmem = pl.BlockSpec(memory_space=pltpu.VMEM)
    hbm = pl.BlockSpec(memory_space=pltpu.HBM)
    remote = each * (n - 1)
    final_gate, final_up, scale_gate, scale_up, routed = pl.pallas_call(
        functools.partial(exchange, groups, n, each, rows, width),
        out_shape=(final, final, scale, scale, jax.ShapeDtypeStruct((groups, columns, n * rows), jnp.bfloat16)),
        in_specs=[hbm] * 4 + [vmem],
        out_specs=(hbm, hbm, vmem, vmem, vmem),
        scratch_shapes=[
            land,
            land,
            pltpu.SemaphoreType.DMA((each, 2)),
            pltpu.VMEM((remote, 2, rows, width), jnp.bfloat16),
            pltpu.VMEM((SLOTS, 2, rows, width), jnp.float32),
            pltpu.VMEM((SLOTS, 2, rows, width), jnp.bfloat16),
            pltpu.SemaphoreType.DMA((SLOTS, 2, 2)),
            pltpu.SemaphoreType.DMA((remote, 2)),
            pltpu.SemaphoreType.DMA((each, 2, n)),
            pltpu.SemaphoreType.DMA((n - 1,)),
            pltpu.SemaphoreType.DMA((n - 1,)),
            pltpu.SemaphoreType.DMA((groups - 1,)),
            pltpu.SemaphoreType.DMA((groups - 1,)),
        ],
        compiler_params=pltpu.CompilerParams(
            collective_id=0, has_side_effects=True, vmem_limit_bytes=60 * 1024 * 1024
        ),
    )(master_gate, second_gate, master_up, second_up, router)
    serve_router = routed.reshape(groups * columns, n * rows).T
    return (
        final_gate, final_up,
        scale_gate.reshape(each, width), scale_up.reshape(each, width), serve_router,
    )


def solution(mesh):
    groups, n = mesh.shape["expert"], mesh.shape["shard"]
    in_specs = (
        P("expert", "shard", None),
        P("expert", "shard", None),
        P("expert", "shard", None),
        P("expert", "shard", None),
        P("shard", "expert"),
        P("shard"),
    )
    out_specs = (
        P(("expert", "shard"), None, None),
        P(("expert", "shard"), None, None),
        P(("expert", "shard"), None),
        P(("expert", "shard"), None),
        P(),
    )
    return jax.shard_map(
        functools.partial(shards, groups, n), mesh=mesh, in_specs=in_specs, out_specs=out_specs, check_vma=False
    )
```

```python
import functools

import jax
import jax.numpy as jnp
from jax import lax
from jax.experimental import pallas as pl
from jax.experimental.pallas import tpu as pltpu
from jax.sharding import PartitionSpec as P

MESH = pl.DeviceIdType.MESH
SLOTS = 3
DELIVER_MIB = 4
STRIP = 64


def exchange(
    groups, n, each, rows, width,
    master_gate, second_gate, master_up, second_up, router,
    land_gate, land_up, scale_gate, scale_up, routed,
    sent, wide, narrow, in_sem, send_sem, recv_sem, row_send, row_recv, col_send, col_recv,
):
    group, me = lax.axis_index("expert"), lax.axis_index("shard")
    half = n // 2
    near = half - 2
    n_remote = each * (n - 1)
    n_items = each * n
    base = (me // half) * half
    chip = me // 2
    outer = ((chip == 0) | (chip == half - 1)).astype(jnp.int32)

    def item(i):
        late = outer * (each * (near + 1))
        q = i - late
        own = i >= n_remote
        early = (i < late) & (outer == 1)
        span = n - 1
        k = jnp.where(outer == 1, jnp.where(early, half + lax.rem(i, near + 1), lax.rem(q + span * half, half)), lax.rem(i, span))
        j = jnp.where(outer == 1, jnp.where(early, i // (near + 1), q // half), i // span)
        cross_to = lax.rem(base + half + lax.rem(k + me, half), n)
        near_to = base + lax.rem((me - base) // 2 * 2 + 2 + lax.rem(k + half, near), half)
        pair_to = me + 1 - 2 * lax.rem(me, 2)
        target = jnp.where(own, me, jnp.where(k < half, cross_to, jnp.where(k < half + near, near_to, pair_to)))
        return target, jnp.where(own, i - n_remote, j)

    sources = ((master_gate, second_gate), (master_up, second_up))
    lands = (land_gate, land_up)

    def reads(i):
        target, j = item(i)
        slot = lax.rem(i, SLOTS)
        e = target * each + j
        return [
            pltpu.make_async_copy(ref.at[e], held.at[slot, t], in_sem.at[slot, t, k])
            for t in range(2)
            for k, (ref, held) in enumerate(zip(sources[t], (wide, narrow)))
        ]

    def my_rows():
        return pl.ds(pl.multiple_of(me * rows, rows), rows)

    def sends(i):
        target, j = item(i)
        return [
            pltpu.make_async_remote_copy(
                src_ref=sent.at[i, t],
                dst_ref=lands[t].at[j, my_rows()],
                send_sem=send_sem.at[i, t],
                recv_sem=recv_sem.at[j, t, me],
                device_id=(group, target),
                device_id_type=MESH,
            )
            for t in range(2)
        ]

    for i in range(SLOTS):
        for copy in reads(jnp.int32(i)):
            copy.start()

    barrier = pltpu.get_barrier_semaphore()
    for k in range(1, n):
        pl.semaphore_signal(barrier, inc=1, device_id=(group, lax.rem(me + k, n)), device_id_type=MESH)
    for k in range(1, groups):
        pl.semaphore_signal(barrier, inc=1, device_id=(lax.rem(group + k, groups), me), device_id_type=MESH)
    pl.semaphore_wait(barrier, n + groups - 2)

    def row_copy(k):
        return pltpu.make_async_remote_copy(
            src_ref=router,
            dst_ref=routed.at[group, :, my_rows()],
            send_sem=row_send.at[k],
            recv_sem=row_recv.at[k],
            device_id=(group, lax.rem(me + k + 1, n)),
            device_id_type=MESH,
        )

    def col_copy(k):
        return pltpu.make_async_remote_copy(
            src_ref=routed.at[group],
            dst_ref=routed.at[group],
            send_sem=col_send.at[k],
            recv_sem=col_recv.at[k],
            device_id=(lax.rem(group + k + 1, groups), me),
            device_id_type=MESH,
        )

    for k in range(n - 1):
        row_copy(k).start()
    routed[group, :, my_rows()] = router[...]

    def merge(i, put):
        slot = lax.rem(i, SLOTS)
        for t in range(2):
            def strip(s, carry, t=t):
                at = pl.ds(pl.multiple_of(s * STRIP, STRIP), STRIP)
                total = wide[slot, t, at, :] + narrow[slot, t, at, :].astype(jnp.float32)
                put(t, s, total.astype(jnp.bfloat16))
                return carry
            lax.fori_loop(0, rows // STRIP, strip, 0)

    def produce(i, carry):
        for copy in reads(i):
            copy.wait()

        @pl.when(i < n_remote)
        def _():
            def put(t, s, value):
                sent[i, t, pl.ds(pl.multiple_of(s * STRIP, STRIP), STRIP), :] = value
            merge(i, put)

        @pl.when(i >= n_remote)
        def _():
            def put(t, s, value):
                lands[t][i - n_remote, pl.ds(pl.multiple_of(me * rows + s * STRIP, STRIP), STRIP), :] = value
            merge(i, put)

        @pl.when(i + SLOTS < n_items)
        def _():
            for copy in reads(i + SLOTS):
                copy.start()

        @pl.when((i >= 1) & (i <= n_remote))
        def _():
            for copy in sends(i - 1):
                copy.start()
        return carry

    lax.fori_loop(0, n_items, produce, 0)

    for k in range(n - 1):
        row_copy(k).wait()
    for k in range(groups - 1):
        col_copy(k).start()

    scales = (scale_gate, scale_up)

    def arrive(j, t):
        def one(k, c):
            source = lax.rem(me + 1 + k, n)
            pltpu.make_async_remote_copy(
                src_ref=sent.at[0, t],
                dst_ref=lands[t].at[j, pl.ds(pl.multiple_of(source * rows, rows), rows)],
                send_sem=send_sem.at[0, t],
                recv_sem=recv_sem.at[j, t, source],
                device_id=(group, source),
                device_id_type=MESH,
            ).wait_recv()
            return c

        lax.fori_loop(0, n - 1, one, 0)

    def finish(j, carry):
        for t in range(2):
            arrive(j, t)
            scales[t][j] = normalise(lands[t].at[j], lands[t].at[j])
        return carry

    lax.fori_loop(0, each, finish, 0)

    for k in range(groups - 1):
        col_copy(k).wait()
    def drain(i, carry):
        for copy in sends(i):
            copy.wait_send()
        return carry

    lax.fori_loop(0, n_remote, drain, 0)


def normalise(source, target):
    depth, width = source.shape

    def add(s, total):
        block = jnp.abs(source[pl.ds(pl.multiple_of(s * STRIP, STRIP), STRIP), :].astype(jnp.float32))
        return total + jnp.sum(block.reshape(STRIP // 8, 8, width), axis=0)

    total = lax.fori_loop(0, depth // STRIP, add, jnp.zeros((8, width), jnp.float32))
    scale = jnp.sum(total, axis=0, keepdims=True) / depth
    factor = jnp.broadcast_to(1.0 / scale, (STRIP, width))

    def divide(s, c):
        at = pl.ds(pl.multiple_of(s * STRIP, STRIP), STRIP)
        target[at, :] = (source[at, :].astype(jnp.float32) * factor).astype(jnp.bfloat16)
        return c

    lax.fori_loop(0, depth // STRIP, divide, 0)
    return scale


def deliver(
    each, land_gate, land_up, part_gate, part_up, routed,
    final_gate, final_up, scale_gate, scale_up, serve_router,
    turned, sem, turned_sem,
):
    tensors = ((land_gate, part_gate, final_gate, scale_gate), (land_up, part_up, final_up, scale_up))
    copies = [
        pltpu.make_async_copy(tensors[t][0].at[j], tensors[t][2].at[j], sem.at[j, t])
        for j in range(each)
        for t in range(2)
    ]
    for copy in copies:
        copy.start()
    for t, (land, part, final, scale) in enumerate(tensors):
        for j in range(each):
            scale[j:j + 1, :] = part[j]
    side = routed.shape[0]
    for c in range(routed.shape[1] // side):
        at = slice(c * side, (c + 1) * side)
        turned[at, :] = routed[:, at].astype(jnp.float32).T.astype(jnp.bfloat16)
    copy = pltpu.make_async_copy(turned, serve_router, turned_sem.at[0])
    copy.start()
    copies.append(copy)
    for copy in copies:
        copy.wait()


def shards(groups, n, master_gate, second_gate, master_up, second_up, router_weight, router_gain):
    experts, rows, width = master_gate.shape
    each = experts // n
    columns = router_weight.shape[1]
    router = (router_weight * router_gain[:, None]).astype(jnp.bfloat16).T
    land = pltpu.VMEM((each, n * rows, width), jnp.bfloat16)
    final = jax.ShapeDtypeStruct((each, n * rows, width), jnp.bfloat16)
    scale = pltpu.VMEM((each, 1, width), jnp.float32)
    vmem = pl.BlockSpec(memory_space=pltpu.VMEM)
    hbm = pl.BlockSpec(memory_space=pltpu.HBM)
    remote = each * (n - 1)
    land_gate, land_up, part_gate, part_up, routed = pl.pallas_call(
        functools.partial(exchange, groups, n, each, rows, width),
        out_shape=(land, land, scale, scale, pltpu.VMEM((groups, columns, n * rows), jnp.bfloat16)),
        in_specs=[hbm] * 4 + [vmem],
        out_specs=(vmem,) * 5,
        scratch_shapes=[
            pltpu.VMEM((remote, 2, rows, width), jnp.bfloat16),
            pltpu.VMEM((SLOTS, 2, rows, width), jnp.float32),
            pltpu.VMEM((SLOTS, 2, rows, width), jnp.bfloat16),
            pltpu.SemaphoreType.DMA((SLOTS, 2, 2)),
            pltpu.SemaphoreType.DMA((remote, 2)),
            pltpu.SemaphoreType.DMA((each, 2, n)),
            pltpu.SemaphoreType.DMA((n - 1,)),
            pltpu.SemaphoreType.DMA((n - 1,)),
            pltpu.SemaphoreType.DMA((groups - 1,)),
            pltpu.SemaphoreType.DMA((groups - 1,)),
        ],
        compiler_params=pltpu.CompilerParams(
            collective_id=0, has_side_effects=True, vmem_limit_bytes=32 * 1024 * 1024
        ),
    )(master_gate, second_gate, master_up, second_up, router)
    experts_all, model = groups * columns, n * rows
    total = jax.ShapeDtypeStruct((each, width), jnp.float32)
    return pl.pallas_call(
        functools.partial(deliver, each),
        out_shape=(final, final, total, total, jax.ShapeDtypeStruct((model, experts_all), jnp.bfloat16)),
        in_specs=[pl.BlockSpec(memory_space=pl.ANY)] * 2 + [vmem] * 3,
        out_specs=(hbm, hbm, vmem, vmem, hbm),
        scratch_shapes=[
            pltpu.VMEM((model, experts_all), jnp.bfloat16),
            pltpu.SemaphoreType.DMA((each, 2)),
            pltpu.SemaphoreType.DMA((1,)),
        ],
        compiler_params=pltpu.CompilerParams(vmem_limit_bytes=DELIVER_MIB * 1024 * 1024),
    )(land_gate, land_up, part_gate, part_up, routed.reshape(experts_all, model))


def solution(mesh):
    groups, n = mesh.shape["expert"], mesh.shape["shard"]
    in_specs = (
        P("expert", "shard", None),
        P("expert", "shard", None),
        P("expert", "shard", None),
        P("expert", "shard", None),
        P("shard", "expert"),
        P("shard"),
    )
    out_specs = (
        P(("expert", "shard"), None, None),
        P(("expert", "shard"), None, None),
        P(("expert", "shard"), None),
        P(("expert", "shard"), None),
        P(),
    )
    return jax.shard_map(
        functools.partial(shards, groups, n), mesh=mesh, in_specs=in_specs, out_specs=out_specs, check_vma=False
    )
```
